256 devices in a mesh: section: 16 (over y, z_hi, core), dp: 16 (over x, z_lo).
Axes of the slice: x: 4, y: 4, z: 8 (z_hi: 2, z_lo: 4; z = z_hi * 4 + z_lo), core: 2. Of those that a mesh axis runs over, the one named last changes fastest.
Arguments:
- student_states: bfloat16 [16, 2048, 2048], P('section', 'dp'), may hold values from -6 to 6
- teacher_states: bfloat16 [64, 2048, 7168], P('section', 'dp'), may hold values from -18 to 18
- projector: bfloat16 [16, 2048, 7168], P('section', None, 'dp'), may hold values from -0.125 to 0.125
- layer_map: int32 [16], replicated, may hold values from 0 to 60, as said below
- boundaries: int32 [17], replicated, may hold values from 0 to 61, as said below
- valid_counts: int32 [16], P('dp'), may hold values from 32 to 128, as said below
Outputs:
- student_grads: bfloat16 [16, 2048, 2048], P('section', 'dp')
- projector_grads: bfloat16 [16, 2048, 7168], P('section', None, 'dp')
- layer_losses: float32 [16], P('section')
The draws below stay inside these ranges and needn't reach their ends.
Inputs may be any that keep to these rules, and one draw needn't show every extreme that they name: Section k holds 4 or 3 teacher layers, three sections the smaller number; boundaries[0] is 0 and boundaries[16] is 61. Teacher layer layer_map[l] lies on a section from l - 2 to l + 2; student layers 0 and 15 pair with layers of sections 1 and 14, student layers 1 and 14 with layers of sections 3 and 12. `valid_counts`: the valid tokens stand first in their micro-batch; the last micro-batch is full.
All inputs are finite; a program needn't handle non-finite values.
Results may differ from the reference program's by a relative error of at most 0.015.
Values may be sent and summed in bfloat16 or wider, within the bound.
No kernel may reach another device: no remote copies, remote signals or barrier semaphores. Data moves between devices by JAX's collectives and lax.ppermute only.
A program may use at most 128 MiB of HBM per device.

```python
import jax
import jax.numpy as jnp
from jax import lax

DS = 2048
DT = 7168
MB_TOK = 128
TL_DEV = 4
STUDENT_LAYERS = 16
SLOTS = 64
TOKENS = 2048
N_SECTION = 16
N_DP = 16


def section_plan(key):
    base = jax.random.fold_in(key, 17)
    first_key = jax.random.fold_in(base, 1)
    second_key = jax.random.fold_in(base, 2)
    third_key = jax.random.fold_in(base, 3)
    places = jnp.arange(N_SECTION, dtype=jnp.int32)
    shorter = (jax.random.permutation(first_key, N_SECTION) < 3).astype(jnp.int32)
    held = TL_DEV - shorter
    bounds = jnp.concatenate([jnp.zeros((1,), jnp.int32), jnp.cumsum(held).astype(jnp.int32)])
    offsets = jax.random.randint(second_key, (N_SECTION,), -2, 3).astype(jnp.int32)
    owners = jnp.clip(places + offsets, 0, N_SECTION - 1)
    owners = owners.at[1].set(3).at[N_SECTION - 2].set(N_SECTION - 4)
    owners = owners.at[0].set(1).at[N_SECTION - 1].set(N_SECTION - 2)
    within = jax.random.randint(third_key, (N_SECTION,), 0, TL_DEV).astype(jnp.int32) % held[owners]
    mapped = (bounds[owners] + within).astype(jnp.int32)
    return (bounds, mapped)


def draw_layer_map(key, part):
    return section_plan(key)[1]


def draw_boundaries(key, part):
    return section_plan(key)[0]


def draw_valid_counts(key, part):
    places = jnp.arange(N_DP, dtype=jnp.int32)
    lowest = MB_TOK // 4
    rising = lowest + (MB_TOK - lowest) * places // max(N_DP - 1, 1)
    jitter = jax.random.randint(jax.random.fold_in(key, 5), (N_DP,), 0, MB_TOK // 8 + 1).astype(jnp.int32)
    counts = jnp.clip(rising - jitter, lowest, MB_TOK).astype(jnp.int32)
    return counts.at[N_DP - 1].set(MB_TOK)


def levels(key, extent, pieces, least, largest):
    level = 1.0
    for position, shards_of in pieces:
        heights = jax.random.uniform(jax.random.fold_in(jax.random.fold_in(key, 6), position), (shards_of,), jnp.float32, least / len(pieces), largest / len(pieces))
        level = level * jnp.repeat(jnp.exp(heights), extent[position] // shards_of).reshape((-1,) + (1,) * (len(extent) - 1 - position))
    return level


def normal_values(stream_key, shape, scale, most, shards=(), kind=jnp.bfloat16):
    values = jax.random.normal(stream_key, shape, jnp.float32) * scale
    if len(shards) > 0:
        values = levels(stream_key, shape, shards, -0.22, 0.18) * values
    return jnp.clip(values, min=-most, max=most).astype(kind)


def setup_inputs(seed: int = 0) -> dict:
    streams_of = jax.random.split(jax.random.key(seed), 7)
    student_states = normal_values(streams_of[0], (STUDENT_LAYERS, TOKENS, DS), 1.0, 6.0, ((0, 16), (1, 16)))
    teacher_states = normal_values(streams_of[1], (SLOTS, TOKENS, DT), 3.0, 18.0, ((0, 16), (1, 16)))
    projector = normal_values(streams_of[2], (STUDENT_LAYERS, DS, DT), DS ** -0.5, 0.125, ((0, 16), (2, 16)))
    layer_map = draw_layer_map(jax.random.fold_in(streams_of[6], 71), 0)
    boundaries = draw_boundaries(jax.random.fold_in(streams_of[6], 71), 0)
    valid_counts = draw_valid_counts(jax.random.fold_in(streams_of[6], 71), 0)
    return dict(student_states=student_states, teacher_states=teacher_states, projector=projector, layer_map=layer_map, boundaries=boundaries, valid_counts=valid_counts)


loss_scale = 128.0
norm_eps = 1e-06

def reference(student_states, teacher_states, projector, layer_map, boundaries, valid_counts):
    rows = jnp.arange(TOKENS, dtype=jnp.int32)
    limit = valid_counts[rows // MB_TOK]
    valid = (rows % MB_TOK < limit).astype(jnp.float32)[:, None]
    total = jnp.sum(valid_counts).astype(jnp.float32)
    owners = lax.optimization_barrier(jnp.sum((boundaries[None, 1:N_SECTION] <= layer_map[:, None]).astype(jnp.int32), axis=1))
    slots = (owners * TL_DEV + layer_map - boundaries[owners]).astype(jnp.int32)
    group_width = DT // N_DP
    student_list = []
    projector_list = []
    loss_list = []
    for layer in range(STUDENT_LAYERS):
        wide = teacher_states[slots[layer]].astype(jnp.float32)
        target = (wide * lax.rsqrt(lax.optimization_barrier(jnp.mean(wide * wide, axis=1, keepdims=True)) + norm_eps)).astype(jnp.bfloat16)
        projected = jnp.dot(student_states[layer], projector[layer], preferred_element_type=jnp.float32)
        residual = projected - target.astype(jnp.float32)
        loss_list.append(jnp.sum(valid * residual * residual) / (total * DT))
        scaled = (valid * (loss_scale / total) * residual).astype(jnp.bfloat16)
        summed = jnp.zeros((TOKENS, DS), jnp.float32)
        for group in range(N_DP):
            left = scaled[:, group * group_width:(group + 1) * group_width]
            right = projector[layer][:, group * group_width:(group + 1) * group_width]
            piece = jnp.dot(left, right.T, preferred_element_type=jnp.float32).astype(jnp.bfloat16)
            summed = summed + piece.astype(jnp.float32)
        student_list.append(summed.astype(jnp.bfloat16))
        projector_list.append(jnp.dot(student_states[layer].T, scaled, preferred_element_type=jnp.float32).astype(jnp.bfloat16))
    return (jnp.stack(student_list), jnp.stack(projector_list), jnp.stack(loss_list))
```

```python
import jax
import jax.numpy as jnp
from jax import lax
from jax.experimental import pallas as pl
from jax.experimental.pallas import tpu as pltpu
from jax.sharding import Mesh
from jax.sharding import PartitionSpec as P

loss_scale = 128.0
norm_eps = 1e-06


SECTION = ("y", "zh", "core")
DP = ("x", "zl")
ROWS = 32


def rotate(block, axis, distance):
    n = lax.axis_size(axis)
    return lax.ppermute(block, axis, [(i, (i + distance) % n) for i in range(n)])


def exchange(block, axis, bit):
    n = lax.axis_size(axis)
    return lax.ppermute(block, axis, [(i, i ^ bit) for i in range(n)])


def prepare_body(places, order, rows, out):
    wide = rows[0].astype(jnp.float32)
    scale = lax.rsqrt(jnp.mean(wide * wide, axis=1, keepdims=True) + norm_eps)
    chunks, zs = out.shape[1], out.shape[2]
    group = wide.shape[1] // order.shape[0]
    width = group // zs
    for chunk in range(chunks):
        halves = []
        for half in range(2):
            start = pl.multiple_of(order[2 * chunk + half] * group, group)
            piece = rows[0, :, pl.ds(start, group)].astype(jnp.float32)
            halves.append((piece * scale).astype(jnp.bfloat16))
        for z in range(zs):
            cut = slice(z * width, (z + 1) * width)
            out[0, chunk, z] = jnp.concatenate([h[:, cut] for h in halves], axis=1)


def prepare(teacher, places, order):
    _, tokens, features = teacher.shape
    pieces = places.shape[0]
    rows = min(ROWS, tokens)
    wide = features // 8
    return pl.pallas_call(
        prepare_body,
        out_shape=jax.ShapeDtypeStruct((pieces, 2, 4, tokens, wide), jnp.bfloat16),
        grid_spec=pltpu.PrefetchScalarGridSpec(
            num_scalar_prefetch=2,
            grid=(pieces, tokens // rows),
            in_specs=[pl.BlockSpec((1, rows, features), lambda k, i, places, order: (places[k], i, 0))],
            out_specs=pl.BlockSpec((1, 2, 4, rows, wide), lambda k, i, places, order: (k, 0, 0, i, 0)),
        ),
        compiler_params=pltpu.CompilerParams(dimension_semantics=("arbitrary", "arbitrary")),
    )(places, order, teacher)


def dot(a, b, ca, cb):
    return lax.dot_general(a, b, (((ca,), (cb,)), ((), ())), preferred_element_type=jnp.float32)


def per_device(student_states, teacher_states, projector, layer_map, boundaries, valid_counts):
    y, zh, core = (lax.axis_index(a) for a in SECTION)
    x, zl = (lax.axis_index(a) for a in DP)
    sections = lax.axis_size(SECTION)
    chip = 2 * y + zh
    here = 2 * chip + core
    student, weights = student_states[0], projector[0]

    owners = jnp.sum((boundaries[None, 1:sections] <= layer_map[:, None]).astype(jnp.int32), axis=1)
    layers = jnp.arange(sections, dtype=jnp.int32)

    across = 2 * (2 * y + 1 - zh) + core
    beyond = jnp.where(zh == 0, 2 * (chip - 1), 2 * (chip + 1)) + core
    aside = jnp.where(core == 1, 2 * (chip + 1), 2 * chip - 1)
    sibling = 2 * chip + 1 - core
    wanted = jnp.stack([sibling, aside, here, across, beyond])
    hit = layers[None, :] == wanted[:, None]
    owner_of = jnp.sum(jnp.where(hit, owners[None, :], 0), axis=1)
    first = jnp.sum(jnp.where(jnp.arange(sections + 1) == here, boundaries, 0))
    places = jnp.sum(jnp.where(hit, layer_map[None, :], 0), axis=1) - first
    places = jnp.clip(places, 0, teacher_states.shape[0] - 1)
    order = jnp.stack([(x + 2) % 4, (x + 1) % 4, (x + 3) % 4, x]).astype(jnp.int32)
    own_owner, across_owner, beyond_owner = owner_of[2], owner_of[3], owner_of[4]
    own_here = own_owner == here
    across_here = across_owner == here
    beyond_here = beyond_owner == here
    across_near = across_owner // 2 == chip
    own_near = own_owner // 2 == chip

    students = [student] + [rotate(student, "zl", k) for k in (1, 2, 3)]
    half = weights.shape[0] // 2
    w_prev = rotate(weights, "x", 1)
    w_next = rotate(weights, "x", -1)

    mine = jnp.broadcast_to(valid_counts, (128,))
    counts = [mine] + [rotate(mine, "zl", k) for k in (1, 2, 3)]
    total = counts[0] + counts[1] + counts[2] + counts[3]
    total = total + exchange(total, "x", 1)
    total = total + exchange(total, "x", 2)

    given = prepare(teacher_states, places[:2], order)
    kept = prepare(teacher_states, places[2:], order)
    from_sibling = exchange(given, "core", 1)

    y_route = [((i, 0), (i - 1, 0)) for i in range(1, 4)] + [((i, 1), (i + 1, 1)) for i in range(3)]
    y_route = [(a * 2 + b, c * 2 + d) for (a, b), (c, d) in y_route]
    relayed = []
    for chunk in range(2):
        moved = jnp.where(beyond_here, kept[2, chunk], from_sibling[1, chunk])
        relayed.append(lax.ppermute(moved, ("y", "zh"), y_route))

    def slab(array, index):
        return lax.dynamic_index_in_dim(array, index, 0, keepdims=False)

    targets = []
    for chunk in range(2):
        blocks = []
        for k in range(4):
            place = (zl + k) % 4
            own = jnp.where(own_here, slab(kept[0, chunk], place), slab(from_sibling[0, chunk], place))
            if k:
                own = rotate(own, "zl", k)
            cross = jnp.where(
                across_near,
                jnp.where(across_here, slab(kept[1, chunk], place), slab(from_sibling[1, chunk], place)),
                slab(relayed[chunk], place),
            )
            route = [(h * 4 + z, (1 - h) * 4 + (z + k) % 4) for h in range(2) for z in range(4)]
            cross = lax.ppermute(cross, ("zh", "zl"), route)
            blocks.append(jnp.where(own_near, own, cross))
        targets.append(blocks)

    w_opp_top = rotate(w_prev[:half], "x", 1)
    w_opp_bot = rotate(w_next[half:], "x", -1)
    w_opp = jnp.concatenate([w_opp_top, w_opp_bot], axis=0)

    per_batch = student.shape[0]
    token = jnp.arange(per_batch, dtype=jnp.int32)
    valid = jnp.concatenate([token < c[0] for c in counts])[:, None].astype(jnp.float32)
    count = total[0].astype(jnp.float32)
    factor = valid * (loss_scale / count)
    rows = jnp.concatenate(students, axis=0)
    width = weights.shape[1]

    squares = 0.0
    scaled = []
    for index, w in enumerate((w_opp, w_next, w_prev, weights)):
        chunk, side = divmod(index, 2)
        target = jnp.concatenate(
            [t[:, side * width : (side + 1) * width] for t in targets[chunk]], axis=0
        )
        residual = dot(rows, w, 1, 0) - target.astype(jnp.float32)
        squares = squares + jnp.sum(valid * residual * residual)
        scaled.append((factor * residual).astype(jnp.bfloat16))

    top, bot = rows[:, :half], rows[:, half:]

    def grad(part, s):
        return dot(part, s, 0, 0)

    up_top = rotate(grad(top, scaled[0]).astype(jnp.bfloat16), "x", 2 - 1)
    down_bot = rotate(grad(bot, scaled[0]).astype(jnp.bfloat16), "x", -1)
    next_bot = rotate(grad(bot, scaled[1]).astype(jnp.bfloat16), "x", 1)
    next_top = rotate((grad(top, scaled[1]) + up_top.astype(jnp.float32)).astype(jnp.bfloat16), "x", 1)
    prev_top = rotate(grad(top, scaled[2]).astype(jnp.bfloat16), "x", -1)
    prev_bot = rotate((grad(bot, scaled[2]) + down_bot.astype(jnp.float32)).astype(jnp.bfloat16), "x", -1)

    student_part = dot(scaled[0], w_opp, 1, 1)
    for s, w in zip(scaled[1:], (w_next, w_prev, weights)):
        student_part = student_part + dot(s, w, 1, 1)
    student_grad = student_part[:per_batch]
    for k in (1, 2, 3):
        part = student_part[k * per_batch : (k + 1) * per_batch].astype(jnp.bfloat16)
        student_grad = student_grad + rotate(part, "zl", -k).astype(jnp.float32)
    student_grad = student_grad.astype(jnp.bfloat16)

    own_top = grad(top, scaled[3]) + next_top.astype(jnp.float32) + prev_top.astype(jnp.float32)
    own_bot = grad(bot, scaled[3]) + next_bot.astype(jnp.float32) + prev_bot.astype(jnp.float32)
    projector_grad = jnp.concatenate([own_top, own_bot], axis=0).astype(jnp.bfloat16)

    squares = jnp.broadcast_to(squares, (128,))
    for axis in ("zl", "x"):
        for bit in (1, 2):
            squares = squares + exchange(squares, axis, bit)
    teacher_width = width * lax.axis_size(DP)
    loss = squares[:1] / (count * teacher_width)
    return (student_grad[None], projector_grad[None], loss)


def solution(mesh):
    split = Mesh(mesh.devices.reshape(4, 2, 2, 4, 4), SECTION + DP)
    return jax.shard_map(
        per_device,
        mesh=split,
        in_specs=(
            P(SECTION, DP, None),
            P(SECTION, DP, None),
            P(SECTION, None, DP),
            P(),
            P(),
            P(DP),
        ),
        out_specs=(P(SECTION, DP, None), P(SECTION, None, DP), P(SECTION)),
        check_vma=False,
    )
```

```python
import jax
import jax.numpy as jnp
from jax import lax
from jax.experimental import pallas as pl
from jax.experimental.pallas import tpu as pltpu
from jax.sharding import Mesh
from jax.sharding import PartitionSpec as P

loss_scale = 128.0
norm_eps = 1e-06


SECTION = ("y", "zh", "core")
DP = ("x", "zl")
ROWS = 32


def rotate(block, axis, distance):
    n = lax.axis_size(axis)
    return lax.ppermute(block, axis, [(i, (i + distance) % n) for i in range(n)])


def exchange(block, axis, bit):
    n = lax.axis_size(axis)
    return lax.ppermute(block, axis, [(i, i ^ bit) for i in range(n)])


def prepare_body(places, order, limit, rows, out):
    wide = rows[0].astype(jnp.float32)
    scale = lax.rsqrt(jnp.mean(wide * wide, axis=1, keepdims=True) + norm_eps)
    token = pl.program_id(1) * wide.shape[0] + lax.broadcasted_iota(jnp.int32, scale.shape, 0)
    scale = jnp.where(token < limit[0], scale, 0.0)
    chunks, zs = out.shape[1], out.shape[2]
    group = wide.shape[1] // order.shape[0]
    width = group // zs
    for chunk in range(chunks):
        halves = []
        for half in range(2):
            start = pl.multiple_of(order[2 * chunk + half] * group, group)
            piece = rows[0, :, pl.ds(start, group)].astype(jnp.float32)
            halves.append((piece * scale).astype(jnp.bfloat16))
        for z in range(zs):
            cut = slice(z * width, (z + 1) * width)
            out[0, chunk, z] = jnp.concatenate([h[:, cut] for h in halves], axis=1)


def prepare(teacher, places, order, limit):
    _, tokens, features = teacher.shape
    pieces = places.shape[0]
    rows = min(ROWS, tokens)
    wide = features // 8
    return pl.pallas_call(
        prepare_body,
        out_shape=jax.ShapeDtypeStruct((pieces, 2, 4, tokens, wide), jnp.bfloat16),
        grid_spec=pltpu.PrefetchScalarGridSpec(
            num_scalar_prefetch=3,
            grid=(pieces, tokens // rows),
            in_specs=[pl.BlockSpec((1, rows, features), lambda k, i, places, order, limit: (places[k], i, 0))],
            out_specs=pl.BlockSpec((1, 2, 4, rows, wide), lambda k, i, places, order, limit: (k, 0, 0, i, 0)),
        ),
        compiler_params=pltpu.CompilerParams(dimension_semantics=("arbitrary", "arbitrary")),
    )(places, order, limit, teacher)


def dot(a, b, ca, cb):
    return lax.dot_general(a, b, (((ca,), (cb,)), ((), ())), preferred_element_type=jnp.float32)


def compute(student_states, teacher_states, projector, layer_map, boundaries, valid_counts):
    y, zh, core = (lax.axis_index(a) for a in SECTION)
    x, zl = (lax.axis_index(a) for a in DP)
    sections = lax.axis_size(SECTION)
    chip = 2 * y + zh
    here = 2 * chip + core
    weights = projector[0]
    tokens = student_states.shape[1]
    half = weights.shape[0] // 2
    width = weights.shape[1]

    valid = lax.broadcasted_iota(jnp.int32, (tokens, 1), 0) < valid_counts[0]
    student = jnp.where(valid, student_states[0], 0)
    students = [student]
    for k in (1, 2, 3):
        students.append(rotate(student, "zl", k))
    w_prev = rotate(weights, "x", 1)
    w_next = rotate(weights, "x", -1)

    owners = jnp.sum((boundaries[None, 1:sections] <= layer_map[:, None]).astype(jnp.int32), axis=1)
    layers = jnp.arange(sections, dtype=jnp.int32)
    across = 2 * (2 * y + 1 - zh) + core
    beyond = jnp.where(zh == 0, 2 * (chip - 1), 2 * (chip + 1)) + core
    aside = jnp.where(core == 1, 2 * (chip + 1), 2 * chip - 1)
    sibling = 2 * chip + 1 - core
    wanted = jnp.stack([sibling, aside, here, across, beyond])
    hit = layers[None, :] == wanted[:, None]
    owner_of = jnp.sum(jnp.where(hit, owners[None, :], 0), axis=1)
    first = jnp.sum(jnp.where(jnp.arange(sections + 1) == here, boundaries, 0))
    places = jnp.sum(jnp.where(hit, layer_map[None, :], 0), axis=1) - first
    places = jnp.clip(places, 0, teacher_states.shape[0] - 1)
    order = jnp.stack([(x + 2) & 3, (x + 1) & 3, (x + 3) & 3, x]).astype(jnp.int32)
    own_owner, across_owner, beyond_owner = owner_of[2], owner_of[3], owner_of[4]
    own_here = own_owner == here
    across_here = across_owner == here
    beyond_here = beyond_owner == here
    across_near = across_owner >> 1 == chip
    own_near = own_owner >> 1 == chip

    given = prepare(teacher_states, places[:2], order, valid_counts)
    from_sibling = exchange(given, "core", 1)
    kept = prepare(teacher_states, places[2:], order, valid_counts)

    y_route = [((i, 0), (i - 1, 0)) for i in range(1, 4)] + [((i, 1), (i + 1, 1)) for i in range(3)]
    y_route = [(a * 2 + b, c * 2 + d) for (a, b), (c, d) in y_route]
    relayed = []
    for chunk in range(2):
        moved = jnp.where(beyond_here, kept[2, chunk], from_sibling[1, chunk])
        relayed.append(lax.ppermute(moved, ("y", "zh"), y_route))

    def slab(array, index, axis=0):
        return lax.dynamic_index_in_dim(array, index, axis, keepdims=False)

    own = []
    for k in range(4):
        place = (zl + k) & 3
        both = jnp.where(own_here, slab(kept[0], place, 1), slab(from_sibling[0], place, 1))
        own.append(rotate(both, "zl", k) if k else both)
    crossed = []
    for chunk in range(2):
        for k in range(4):
            place = (zl + k) & 3
            cross = jnp.where(
                across_near,
                jnp.where(across_here, slab(kept[1, chunk], place), slab(from_sibling[1, chunk], place)),
                slab(relayed[chunk], place),
            )
            route = [(h * 4 + z, (1 - h) * 4 + (z + k) % 4) for h in range(2) for z in range(4)]
            crossed.append(lax.ppermute(cross, ("zh", "zl"), route))

    w_opp_top = rotate(w_prev[:half], "x", 1)
    w_opp_bot = rotate(w_next[half:], "x", -1)
    rows = jnp.concatenate(students, axis=0)

    w_first = jnp.concatenate([jnp.concatenate([w_opp_top, w_opp_bot], axis=0), w_next], axis=1)
    w_second = jnp.concatenate([w_prev, weights], axis=1)

    def residual_of(chunk, own, w):
        blocks = [jnp.where(own_near, own[k][chunk], crossed[4 * chunk + k]) for k in range(4)]
        target = jnp.concatenate(blocks, axis=0)
        residual = dot(rows, w, 1, 0) - target.astype(jnp.float32)
        return jnp.sum(residual * residual), residual.astype(jnp.bfloat16)

    squares_first, first_res = residual_of(0, own, w_first)
    own, first_res = lax.optimization_barrier((own, first_res))
    pair = dot(rows, first_res, 0, 0).astype(jnp.bfloat16)
    part_first = dot(first_res, w_first, 1, 1)
    up_top = rotate(pair[:half, :width], "x", 1)
    down_bot = rotate(pair[half:, :width], "x", -1)
    squares_second, second_res = residual_of(1, own, w_second)

    sums = jnp.stack([squares_first + squares_second, valid_counts[0].astype(jnp.float32)])
    copies = jnp.broadcast_to(sums, (lax.axis_size(DP), 2))
    sums = jnp.sum(lax.all_to_all(copies, DP, split_axis=0, concat_axis=0, tiled=True), axis=0)
    total = sums[1]
    loss = sums[:1] / (total * (width * lax.axis_size(DP)))
    factor = loss_scale / total

    next_part = pair[:, width:].astype(jnp.float32)
    next_part = jnp.concatenate([next_part[:half] + up_top.astype(jnp.float32), next_part[half:]], axis=0)
    next_part = lax.optimization_barrier((next_part.astype(jnp.bfloat16), sums))[0]
    from_prev = rotate(next_part, "x", 1)
    prev_part = dot(rows, second_res[:, :width], 0, 0)
    prev_part = jnp.concatenate([prev_part[:half], prev_part[half:] + down_bot.astype(jnp.float32)], axis=0)
    prev_part = lax.optimization_barrier((prev_part.astype(jnp.bfloat16), sums))[0]
    from_next = rotate(prev_part, "x", -1)

    student_part = (part_first + dot(second_res, w_second, 1, 1)).astype(jnp.bfloat16)
    student_part = lax.optimization_barrier((student_part, sums))[0]
    returned = []
    for k in (1, 2, 3):
        part = student_part[k * tokens : (k + 1) * tokens]
        returned.append(rotate(part, "zl", -k))

    student_grad = student_part[:tokens].astype(jnp.float32)
    for part in returned:
        student_grad = student_grad + part.astype(jnp.float32)
    student_grad = (student_grad * factor).astype(jnp.bfloat16)
    projector_grad = dot(rows, second_res[:, width:], 0, 0) + from_prev.astype(jnp.float32) + from_next.astype(jnp.float32)
    projector_grad = (projector_grad * factor).astype(jnp.bfloat16)
    return (student_grad[None], projector_grad[None], loss)


def solution(mesh):
    split = Mesh(mesh.devices.reshape(4, 2, 2, 4, 4), SECTION + DP)
    return jax.shard_map(
        compute,
        mesh=split,
        in_specs=(
            P(SECTION, DP, None),
            P(SECTION, DP, None),
            P(SECTION, None, DP),
            P(),
            P(),
            P(DP),
        ),
        out_specs=(P(SECTION, DP, None), P(SECTION, None, DP), P(SECTION)),
        check_vma=False,
    )
```

```python
import jax
import jax.numpy as jnp
from jax import lax
from jax.experimental import pallas as pl
from jax.experimental.pallas import tpu as pltpu
from jax.sharding import Mesh
from jax.sharding import PartitionSpec as P

loss_scale = 128.0
norm_eps = 1e-06


SECTION = ("y", "zh", "core")
DP = ("x", "zl")
ROWS = 32


def rotate(block, axis, distance):
    n = lax.axis_size(axis)
    return lax.ppermute(block, axis, [(i, (i + distance) % n) for i in range(n)])


def exchange(block, axis, bit):
    n = lax.axis_size(axis)
    return lax.ppermute(block, axis, [(i, i ^ bit) for i in range(n)])


def prepare_body(places, order, limit, rows, out):
    wide = rows[0].astype(jnp.float32)
    scale = lax.rsqrt(jnp.mean(wide * wide, axis=1, keepdims=True) + norm_eps)
    token = pl.program_id(1) * wide.shape[0] + lax.broadcasted_iota(jnp.int32, scale.shape, 0)
    scale = jnp.where(token < limit[0], scale, 0.0)
    chunks, zs = out.shape[1], out.shape[2]
    group = wide.shape[1] // order.shape[0]
    width = group // zs
    for chunk in range(chunks):
        halves = []
        for half in range(2):
            start = pl.multiple_of(order[2 * chunk + half] * group, group)
            piece = rows[0, :, pl.ds(start, group)].astype(jnp.float32)
            halves.append((piece * scale).astype(jnp.bfloat16))
        for z in range(zs):
            cut = slice(z * width, (z + 1) * width)
            out[0, chunk, z] = jnp.concatenate([h[:, cut] for h in halves], axis=1)


def prepare(teacher, places, order, limit):
    _, tokens, features = teacher.shape
    pieces = places.shape[0]
    rows = min(ROWS, tokens)
    wide = features // 8
    return pl.pallas_call(
        prepare_body,
        out_shape=jax.ShapeDtypeStruct((pieces, 2, 4, tokens, wide), jnp.bfloat16),
        grid_spec=pltpu.PrefetchScalarGridSpec(
            num_scalar_prefetch=3,
            grid=(pieces, tokens // rows),
            in_specs=[pl.BlockSpec((1, rows, features), lambda k, i, places, order, limit: (places[k], i, 0))],
            out_specs=pl.BlockSpec((1, 2, 4, rows, wide), lambda k, i, places, order, limit: (k, 0, 0, i, 0)),
        ),
        compiler_params=pltpu.CompilerParams(dimension_semantics=("arbitrary", "arbitrary")),
    )(places, order, limit, teacher)


def residual_body(near, projected, *refs):
    own, cross, (out, squares) = refs[:4], refs[4:8], refs[8:]
    rows = cross[0].shape[0]
    total = jnp.zeros((), jnp.float32)
    for k in range(4):
        cut = slice(k * rows, (k + 1) * rows)
        target = jnp.where(near[0] == 1, own[k][0].astype(jnp.float32), cross[k][...].astype(jnp.float32))
        residual = projected[cut] - target
        out[cut] = residual.astype(jnp.bfloat16)
        total = total + jnp.sum(residual * residual)
    squares[0] = total


def residual_of(near, projected, own, chunk, cross):
    tokens = projected.shape[0]
    rows, wide = cross[0].shape

    def whole(shape):
        return pl.BlockSpec(shape, lambda i: (0, 0))

    smem = pl.BlockSpec(memory_space=pltpu.SMEM)
    return pl.pallas_call(
        residual_body,
        out_shape=(
            jax.ShapeDtypeStruct((tokens, wide), jnp.bfloat16),
            jax.ShapeDtypeStruct((1,), jnp.float32),
        ),
        grid=(1,),
        in_specs=[smem, pl.BlockSpec((tokens, wide), lambda i: (0, chunk))]
        + [pl.BlockSpec((1, rows, wide), lambda i: (chunk, 0, 0))] * 4
        + [whole((rows, wide))] * 4,
        out_specs=(whole((tokens, wide)), smem),
    )(near, projected, *own, *cross)


def dot(a, b, ca, cb):
    return lax.dot_general(a, b, (((ca,), (cb,)), ((), ())), preferred_element_type=jnp.float32)


def compute(student_states, teacher_states, projector, layer_map, boundaries, valid_counts):
    y, zh, core = (lax.axis_index(a) for a in SECTION)
    x, zl = (lax.axis_index(a) for a in DP)
    sections = lax.axis_size(SECTION)
    chip = 2 * y + zh
    here = 2 * chip + core
    weights = projector[0]
    tokens = student_states.shape[1]
    half = weights.shape[0] // 2
    width = weights.shape[1]

    valid = lax.broadcasted_iota(jnp.int32, (tokens, 1), 0) < valid_counts[0]
    student = jnp.where(valid, student_states[0], 0)
    students = [student]
    for k in (1, 2, 3):
        students.append(rotate(student, "zl", k))
    w_prev = rotate(weights, "x", 1)
    w_next = rotate(weights, "x", -1)
    w_opp = rotate(weights, "x", 2)

    owners = jnp.sum((boundaries[None, 1:sections] <= layer_map[:, None]).astype(jnp.int32), axis=1)
    layers = jnp.arange(sections, dtype=jnp.int32)
    across = 2 * (2 * y + 1 - zh) + core
    beyond = jnp.where(zh == 0, 2 * (chip - 1), 2 * (chip + 1)) + core
    aside = jnp.where(core == 1, 2 * (chip + 1), 2 * chip - 1)
    sibling = 2 * chip + 1 - core
    wanted = jnp.stack([sibling, aside, here, across, beyond])
    hit = layers[None, :] == wanted[:, None]
    owner_of = jnp.sum(jnp.where(hit, owners[None, :], 0), axis=1)
    first = jnp.sum(jnp.where(jnp.arange(sections + 1) == here, boundaries, 0))
    places = jnp.sum(jnp.where(hit, layer_map[None, :], 0), axis=1) - first
    places = jnp.clip(places, 0, teacher_states.shape[0] - 1)
    order = jnp.stack([(x + 2) & 3, (x + 1) & 3, (x + 3) & 3, x]).astype(jnp.int32)
    own_owner, across_owner, beyond_owner = owner_of[2], owner_of[3], owner_of[4]
    own_here = own_owner == here
    across_here = across_owner == here
    beyond_here = beyond_owner == here
    across_near = across_owner >> 1 == chip
    own_near = own_owner >> 1 == chip

    given = prepare(teacher_states, places[:2], order, valid_counts)
    from_sibling = exchange(given, "core", 1)
    kept = prepare(teacher_states, places[2:], order, valid_counts)

    y_route = [((i, 0), (i - 1, 0)) for i in range(1, 4)] + [((i, 1), (i + 1, 1)) for i in range(3)]
    y_route = [(a * 2 + b, c * 2 + d) for (a, b), (c, d) in y_route]
    moved = jnp.where(beyond_here, kept[2], from_sibling[1])
    relayed = lax.ppermute(moved, ("y", "zh"), y_route)

    def slab(array, index, axis=0):
        return lax.dynamic_index_in_dim(array, index, axis, keepdims=False)

    own = []
    for k in range(4):
        place = (zl + k) & 3
        both = jnp.where(own_here, slab(kept[0], place, 1), slab(from_sibling[0], place, 1))
        own.append(rotate(both, "zl", k) if k else both)
    crossed = []
    for chunk in range(2):
        for k in range(4):
            place = (zl + k) & 3
            cross = jnp.where(
                across_near,
                jnp.where(across_here, slab(kept[1, chunk], place), slab(from_sibling[1, chunk], place)),
                slab(relayed[chunk], place),
            )
            route = [(h * 4 + z, (1 - h) * 4 + (z + k) % 4) for h in range(2) for z in range(4)]
            crossed.append(lax.ppermute(cross, ("zh", "zl"), route))

    rows = jnp.concatenate(students, axis=0)
    w_all = lax.optimization_barrier(jnp.concatenate([w_opp, w_next, w_prev, weights], axis=1))
    projected = lax.optimization_barrier(dot(rows, w_all, 1, 0))
    near = jnp.reshape(own_near.astype(jnp.int32), (1,))
    top, bot = rows[:, :half], rows[:, half:]

    def grad(part, residual):
        return dot(part, residual, 0, 0)

    first_res, squares_first = residual_of(near, projected, own, 0, crossed[:4])
    opp_res, next_res = first_res[:, :width], first_res[:, width:]
    opp_top = grad(top, opp_res).astype(jnp.bfloat16)
    opp_bot = grad(bot, opp_res).astype(jnp.bfloat16)
    next_bot = grad(bot, next_res).astype(jnp.bfloat16)
    up_top = rotate(opp_top, "x", 1)
    down_bot = rotate(opp_bot, "x", -1)
    second_res, squares_second = residual_of(near, projected, own, 1, crossed[4:])

    sums = jnp.stack([squares_first[0] + squares_second[0], valid_counts[0].astype(jnp.float32)])
    copies = jnp.broadcast_to(sums, (lax.axis_size(DP), 2))
    sums = jnp.sum(lax.all_to_all(copies, DP, split_axis=0, concat_axis=0, tiled=True), axis=0)
    total = sums[1]
    loss = sums[:1] / (total * (width * lax.axis_size(DP)))
    factor = loss_scale / total

    next_top = (grad(top, next_res) + up_top.astype(jnp.float32)).astype(jnp.bfloat16)
    next_part = jnp.concatenate([next_top, next_bot], axis=0)
    next_part = lax.optimization_barrier((next_part, sums))[0]
    from_prev = rotate(next_part, "x", 1)
    prev_res, own_res = second_res[:, :width], second_res[:, width:]
    prev_top = grad(top, prev_res).astype(jnp.bfloat16)
    prev_bot = (grad(bot, prev_res) + down_bot.astype(jnp.float32)).astype(jnp.bfloat16)
    prev_part = jnp.concatenate([prev_top, prev_bot], axis=0)
    prev_part = lax.optimization_barrier((prev_part, sums))[0]
    from_next = rotate(prev_part, "x", -1)

    residual = lax.optimization_barrier(jnp.concatenate([first_res, second_res], axis=1))
    student_part = dot(residual, w_all, 1, 1).astype(jnp.bfloat16)
    student_part = lax.optimization_barrier((student_part, sums))[0]
    returned = []
    for k in (1, 2, 3):
        part = student_part[k * tokens : (k + 1) * tokens]
        returned.append(rotate(part, "zl", -k))
    own_part = lax.optimization_barrier(grad(rows, own_res))

    student_grad = student_part[:tokens].astype(jnp.float32)
    for part in returned:
        student_grad = student_grad + part.astype(jnp.float32)
    student_grad = (student_grad * factor).astype(jnp.bfloat16)
    projector_grad = own_part + from_prev.astype(jnp.float32) + from_next.astype(jnp.float32)
    projector_grad = (projector_grad * factor).astype(jnp.bfloat16)
    return (student_grad[None], projector_grad[None], loss)


def solution(mesh):
    split = Mesh(mesh.devices.reshape(4, 2, 2, 4, 4), SECTION + DP)
    return jax.shard_map(
        compute,
        mesh=split,
        in_specs=(
            P(SECTION, DP, None),
            P(SECTION, DP, None),
            P(SECTION, None, DP),
            P(),
            P(),
            P(DP),
        ),
        out_specs=(P(SECTION, DP, None), P(SECTION, None, DP), P(SECTION)),
        check_vma=False,
    )
```

```python
import functools

import jax
import jax.numpy as jnp
from jax import lax
from jax.experimental import pallas as pl
from jax.experimental.pallas import tpu as pltpu
from jax.sharding import Mesh
from jax.sharding import PartitionSpec as P

loss_scale = 128.0
norm_eps = 1e-06


SECTION = ("y", "zh", "core")
DP = ("x", "zl")
ROWS = 32


def rotate(block, axis, distance):
    n = lax.axis_size(axis)
    return lax.ppermute(block, axis, [(i, (i + distance) % n) for i in range(n)])


def exchange(block, axis, bit):
    n = lax.axis_size(axis)
    return lax.ppermute(block, axis, [(i, i ^ bit) for i in range(n)])


PIECES = ("beyond", "across", "here")
ORDER, ZL, LIMIT = 6, 10, 11


def prepare_body(piece, info, mine, theirs, *refs):
    outs, spread = refs[:-1], refs[-1]
    local = info[3 + piece] == 1
    wide = jnp.where(local, mine[0], theirs[0]).astype(jnp.float32)
    scale = lax.rsqrt(jnp.mean(wide * wide, axis=1, keepdims=True) + norm_eps)
    token = pl.program_id(0) * wide.shape[0] + lax.broadcasted_iota(jnp.int32, scale.shape, 0)
    scale = jnp.where(token < info[LIMIT], scale, 0.0)
    group = wide.shape[1] // 4
    width = group // 4
    for chunk in range(2):
        halves = []
        for half in range(2):
            start = pl.multiple_of(info[ORDER + 2 * chunk + half] * group, group)
            cut = pl.ds(start, group)
            part = jnp.where(local, mine[0, :, cut], theirs[0, :, cut]).astype(jnp.float32)
            halves.append((part * scale).astype(jnp.bfloat16))
        for z in range(4):
            cut = slice(z * width, (z + 1) * width)
            spread[chunk, (z - info[ZL]) & 3] = jnp.concatenate([h[:, cut] for h in halves], axis=1)
    for index, out in enumerate(outs):
        out[...] = spread[:, index] if PIECES[piece] == "here" else spread[index]


def prepare(mine, theirs, info, name):
    _, tokens, features = mine.shape
    piece = PIECES.index(name)
    rows = min(ROWS, tokens)
    wide = features // 8
    lead = [(2,)] * 4 if name == "here" else [(4,)] * 2

    def taken(kept):
        def index(i, info):
            on = info[3 + piece] if kept else 1 - info[3 + piece]
            return (info[piece] * on, i * on, 0)

        return pl.BlockSpec((1, rows, features), index)

    def written(dims):
        return pl.BlockSpec((*dims, rows, wide), lambda i, info: (0,) * len(dims) + (i, 0))

    return pl.pallas_call(
        functools.partial(prepare_body, piece),
        out_shape=[jax.ShapeDtypeStruct((*dims, tokens, wide), jnp.bfloat16) for dims in lead],
        grid_spec=pltpu.PrefetchScalarGridSpec(
            num_scalar_prefetch=1,
            grid=(tokens // rows,),
            in_specs=[taken(True), taken(False)],
            out_specs=[written(dims) for dims in lead],
            scratch_shapes=[pltpu.VMEM((2, 4, rows, wide), jnp.bfloat16)],
        ),
        compiler_params=pltpu.CompilerParams(dimension_semantics=("arbitrary",)),
    )(info, mine, theirs)


def residual_body(near, projected, *refs):
    own, cross, (out, squares) = refs[:4], refs[4:8], refs[8:]
    rows = cross[0].shape[0]
    total = jnp.zeros((), jnp.float32)
    for k in range(4):
        cut = slice(k * rows, (k + 1) * rows)
        target = jnp.where(near[0] == 1, own[k][0].astype(jnp.float32), cross[k][...].astype(jnp.float32))
        residual = projected[cut] - target
        out[cut] = residual.astype(jnp.bfloat16)
        total = total + jnp.sum(residual * residual)
    squares[0] = total


def residual_of(near, projected, own, chunk, cross):
    tokens = projected.shape[0]
    rows, wide = cross[0].shape

    def whole(shape):
        return pl.BlockSpec(shape, lambda i: (0, 0))

    smem = pl.BlockSpec(memory_space=pltpu.SMEM)
    return pl.pallas_call(
        residual_body,
        out_shape=(
            jax.ShapeDtypeStruct((tokens, wide), jnp.bfloat16),
            jax.ShapeDtypeStruct((1,), jnp.float32),
        ),
        grid=(1,),
        in_specs=[smem, pl.BlockSpec((tokens, wide), lambda i: (0, chunk))]
        + [pl.BlockSpec((1, rows, wide), lambda i: (chunk, 0, 0))] * 4
        + [whole((rows, wide))] * 4,
        out_specs=(whole((tokens, wide)), smem),
    )(near, projected, *own, *cross)


def dot(a, b, ca, cb):
    return lax.dot_general(a, b, (((ca,), (cb,)), ((), ())), preferred_element_type=jnp.float32)


def compute(student_states, teacher_states, projector, layer_map, boundaries, valid_counts):
    y, zh, core = (lax.axis_index(a) for a in SECTION)
    x, zl = (lax.axis_index(a) for a in DP)
    sections = lax.axis_size(SECTION)
    chip = 2 * y + zh
    here = 2 * chip + core
    weights = projector[0]
    tokens = student_states.shape[1]
    half = weights.shape[0] // 2
    width = weights.shape[1]

    theirs = exchange(teacher_states, "core", 1)

    valid = lax.broadcasted_iota(jnp.int32, (tokens, 1), 0) < valid_counts[0]
    student = jnp.where(valid, student_states[0], 0)
    students = [student]
    for k in (1, 2, 3):
        students.append(rotate(student, "zl", k))
    w_prev = rotate(weights, "x", 1)
    w_next = rotate(weights, "x", -1)
    w_opp = rotate(weights, "x", 2)

    owners = jnp.sum((boundaries[None, 1:sections] <= layer_map[:, None]).astype(jnp.int32), axis=1)
    layers = jnp.arange(sections, dtype=jnp.int32)
    across = 2 * (2 * y + 1 - zh) + core
    beyond = jnp.where(zh == 0, 2 * (chip - 1), 2 * (chip + 1)) + core
    wanted = jnp.stack([beyond, across, here])
    hit = layers[None, :] == wanted[:, None]
    owner_of = jnp.sum(jnp.where(hit, owners[None, :], 0), axis=1)
    layer_of = jnp.sum(jnp.where(hit, layer_map[None, :], 0), axis=1)
    first_of = jnp.sum(jnp.where(layers[None, :] == owner_of[:, None], boundaries[None, :sections], 0), axis=1)
    places = jnp.clip(layer_of - first_of, 0, teacher_states.shape[0] - 1)
    local = (owner_of == here).astype(jnp.int32)
    rest = jnp.stack([(x + 2) & 3, (x + 1) & 3, (x + 3) & 3, x, zl, valid_counts[0]]).astype(jnp.int32)
    info = jnp.concatenate([places, local, rest])
    near = (owner_of >> 1 == chip).astype(jnp.int32)
    across_near = near[1] == 1

    beyond_slabs = prepare(teacher_states, theirs, info, "beyond")
    y_route = [((i, 0), (i - 1, 0)) for i in range(1, 4)] + [((i, 1), (i + 1, 1)) for i in range(3)]
    y_route = [(a * 2 + b, c * 2 + d) for (a, b), (c, d) in y_route]
    relayed = []
    for chunk in range(2):
        relayed.append(lax.ppermute(beyond_slabs[chunk], ("y", "zh"), y_route))
    across_slabs = prepare(teacher_states, theirs, info, "across")

    def send_across(chunk):
        sent = []
        for k in range(4):
            route = [(h * 4 + z, (1 - h) * 4 + (z + k) % 4) for h in range(2) for z in range(4)]
            slab = jnp.where(across_near, across_slabs[chunk][k], relayed[chunk][k])
            sent.append(lax.ppermute(slab, ("zh", "zl"), route))
        return sent

    crossed = send_across(0)
    here_slabs = prepare(teacher_states, theirs, info, "here")
    own = [here_slabs[0]] + [rotate(here_slabs[k], "zl", k) for k in (1, 2, 3)]
    crossed = crossed + send_across(1)

    rows = jnp.concatenate(students, axis=0)
    w_all = lax.optimization_barrier(jnp.concatenate([w_opp, w_next, w_prev, weights], axis=1))
    projected = lax.optimization_barrier(dot(rows, w_all, 1, 0))
    near = near[2:]
    top, bot = rows[:, :half], rows[:, half:]

    def grad(part, residual):
        return dot(part, residual, 0, 0)

    first_res, squares_first = residual_of(near, projected, own, 0, crossed[:4])
    opp_res, next_res = first_res[:, :width], first_res[:, width:]
    opp_top = grad(top, opp_res).astype(jnp.bfloat16)
    opp_bot = grad(bot, opp_res).astype(jnp.bfloat16)
    next_bot = grad(bot, next_res).astype(jnp.bfloat16)
    up_top = rotate(opp_top, "x", 1)
    down_bot = rotate(opp_bot, "x", -1)
    second_res, squares_second = residual_of(near, projected, own, 1, crossed[4:])

    next_top = (grad(top, next_res) + up_top.astype(jnp.float32)).astype(jnp.bfloat16)
    next_part = jnp.concatenate([next_top, next_bot], axis=0)
    from_prev = rotate(next_part, "x", 1)
    prev_res, own_res = second_res[:, :width], second_res[:, width:]
    prev_top = grad(top, prev_res).astype(jnp.bfloat16)
    prev_bot = (grad(bot, prev_res) + down_bot.astype(jnp.float32)).astype(jnp.bfloat16)
    prev_part = jnp.concatenate([prev_top, prev_bot], axis=0)
    from_next = rotate(prev_part, "x", -1)

    residual = lax.optimization_barrier(jnp.concatenate([first_res, second_res], axis=1))
    student_part = dot(residual, w_all, 1, 1).astype(jnp.bfloat16)
    returned = []
    for k in (1, 2, 3):
        part = student_part[k * tokens : (k + 1) * tokens]
        returned.append(rotate(part, "zl", -k))
    own_part = grad(rows, own_res)

    sums = jnp.stack([squares_first[0] + squares_second[0], valid_counts[0].astype(jnp.float32)])
    copies = jnp.broadcast_to(sums, (lax.axis_size(DP), 2))
    copies, own_part = lax.optimization_barrier((copies, own_part))
    sums = jnp.sum(lax.all_to_all(copies, DP, split_axis=0, concat_axis=0, tiled=True), axis=0)
    total = sums[1]
    loss = sums[:1] / (total * (width * lax.axis_size(DP)))
    factor = loss_scale / total

    student_grad = student_part[:tokens].astype(jnp.float32)
    for part in returned:
        student_grad = student_grad + part.astype(jnp.float32)
    student_grad = (student_grad * factor).astype(jnp.bfloat16)
    projector_grad = own_part + from_prev.astype(jnp.float32) + from_next.astype(jnp.float32)
    projector_grad = (projector_grad * factor).astype(jnp.bfloat16)
    return (student_grad[None], projector_grad[None], loss)


def solution(mesh):
    split = Mesh(mesh.devices.reshape(4, 2, 2, 4, 4), SECTION + DP)
    return jax.shard_map(
        compute,
        mesh=split,
        in_specs=(
            P(SECTION, DP, None),
            P(SECTION, DP, None),
            P(SECTION, None, DP),
            P(),
            P(),
            P(DP),
        ),
        out_specs=(P(SECTION, DP, None), P(SECTION, None, DP), P(SECTION)),
        check_vma=False,
    )
```

```python
import functools

import jax
import jax.numpy as jnp
from jax import lax
from jax.experimental import pallas as pl
from jax.experimental.pallas import tpu as pltpu
from jax.sharding import Mesh
from jax.sharding import PartitionSpec as P

loss_scale = 128.0
norm_eps = 1e-06


SECTION = ("y", "zh", "core")
DP = ("x", "zl")
ROWS = 32


def rotate(block, axis, distance):
    n = lax.axis_size(axis)
    return lax.ppermute(block, axis, [(i, (i + distance) % n) for i in range(n)])


def exchange(block, axis, bit):
    n = lax.axis_size(axis)
    return lax.ppermute(block, axis, [(i, i ^ bit) for i in range(n)])


PIECES = ("beyond", "across", "here")
ORDER, ZL, LIMIT = 6, 10, 11


def prepare_body(piece, info, mine, theirs, *refs):
    outs, spread = refs[:-1], refs[-1]
    local = info[3 + piece] == 1
    wide = jnp.where(local, mine[0], theirs[0]).astype(jnp.float32)
    scale = lax.rsqrt(jnp.mean(wide * wide, axis=1, keepdims=True) + norm_eps)
    token = pl.program_id(0) * wide.shape[0] + lax.broadcasted_iota(jnp.int32, scale.shape, 0)
    scale = jnp.where(token < info[LIMIT], scale, 0.0)
    group = wide.shape[1] // 4
    width = group // 4
    for chunk in range(2):
        halves = []
        for half in range(2):
            start = pl.multiple_of(info[ORDER + 2 * chunk + half] * group, group)
            cut = pl.ds(start, group)
            part = jnp.where(local, mine[0, :, cut], theirs[0, :, cut]).astype(jnp.float32)
            halves.append((part * scale).astype(jnp.bfloat16))
        for z in range(4):
            cut = slice(z * width, (z + 1) * width)
            spread[chunk, (z - info[ZL]) & 3] = jnp.concatenate([h[:, cut] for h in halves], axis=1)
    for index, out in enumerate(outs):
        out[...] = spread[index // 4, index % 4] if PIECES[piece] == "here" else spread[index]


def prepare(mine, theirs, info, name):
    _, tokens, features = mine.shape
    piece = PIECES.index(name)
    rows = min(ROWS, tokens)
    wide = features // 8
    lead = [()] * 8 if name == "here" else [(4,)] * 2

    def taken(kept):
        def index(i, info):
            on = info[3 + piece] if kept else 1 - info[3 + piece]
            return (info[piece] * on, i * on, 0)

        return pl.BlockSpec((1, rows, features), index)

    def written(dims):
        return pl.BlockSpec((*dims, rows, wide), lambda i, info: (0,) * len(dims) + (i, 0))

    return pl.pallas_call(
        functools.partial(prepare_body, piece),
        out_shape=[jax.ShapeDtypeStruct((*dims, tokens, wide), jnp.bfloat16) for dims in lead],
        grid_spec=pltpu.PrefetchScalarGridSpec(
            num_scalar_prefetch=1,
            grid=(tokens // rows,),
            in_specs=[taken(True), taken(False)],
            out_specs=[written(dims) for dims in lead],
            scratch_shapes=[pltpu.VMEM((2, 4, rows, wide), jnp.bfloat16)],
        ),
        compiler_params=pltpu.CompilerParams(dimension_semantics=("arbitrary",), vmem_limit_bytes=12 << 20),
    )(info, mine, theirs)


def residual_body(near, projected, *refs):
    own, cross, (out, squares) = refs[:4], refs[4:8], refs[8:]
    rows = cross[0].shape[0]
    total = jnp.zeros((), jnp.float32)
    for k in range(4):
        cut = slice(k * rows, (k + 1) * rows)
        target = jnp.where(near[0] == 1, own[k][...].astype(jnp.float32), cross[k][...].astype(jnp.float32))
        residual = projected[cut] - target
        out[cut] = residual.astype(jnp.bfloat16)
        total = total + jnp.sum(residual * residual)
    squares[0] = total


def residual_of(near, projected, own, chunk, cross):
    tokens = projected.shape[0]
    rows, wide = cross[0].shape

    def whole(shape):
        return pl.BlockSpec(shape, lambda i: (0, 0))

    smem = pl.BlockSpec(memory_space=pltpu.SMEM)
    return pl.pallas_call(
        residual_body,
        out_shape=(
            jax.ShapeDtypeStruct((tokens, wide), jnp.bfloat16),
            jax.ShapeDtypeStruct((1,), jnp.float32),
        ),
        grid=(1,),
        in_specs=[smem, pl.BlockSpec((tokens, wide), lambda i: (0, chunk))]
        + [whole((rows, wide))] * 8,
        out_specs=(whole((tokens, wide)), smem),
        compiler_params=pltpu.CompilerParams(vmem_limit_bytes=16 << 20),
    )(near, projected, *own, *cross)


def dot(a, b, ca, cb):
    return lax.dot_general(a, b, (((ca,), (cb,)), ((), ())), preferred_element_type=jnp.float32)


def compute(student_states, teacher_states, projector, layer_map, boundaries, valid_counts):
    y, zh, core = (lax.axis_index(a) for a in SECTION)
    x, zl = (lax.axis_index(a) for a in DP)
    sections = lax.axis_size(SECTION)
    chip = 2 * y + zh
    here = 2 * chip + core
    weights = projector[0]
    tokens = student_states.shape[1]
    half = weights.shape[0] // 2
    width = weights.shape[1]

    theirs = exchange(teacher_states, "core", 1)

    valid = lax.broadcasted_iota(jnp.int32, (tokens, 1), 0) < valid_counts[0]
    student = jnp.where(valid, student_states[0], 0)
    students = [student]
    for k in (1, 2, 3):
        students.append(rotate(student, "zl", k))
    w_prev = rotate(weights, "x", 1)
    w_next = rotate(weights, "x", -1)
    w_opp = rotate(weights, "x", 2)

    owners = jnp.sum((boundaries[None, 1:sections] <= layer_map[:, None]).astype(jnp.int32), axis=1)
    layers = jnp.arange(sections, dtype=jnp.int32)
    across = 2 * (2 * y + 1 - zh) + core
    beyond = jnp.where(zh == 0, 2 * (chip - 1), 2 * (chip + 1)) + core
    wanted = jnp.stack([beyond, across, here])
    hit = layers[None, :] == wanted[:, None]
    owner_of = jnp.sum(jnp.where(hit, owners[None, :], 0), axis=1)
    layer_of = jnp.sum(jnp.where(hit, layer_map[None, :], 0), axis=1)
    first_of = jnp.sum(jnp.where(layers[None, :] == owner_of[:, None], boundaries[None, :sections], 0), axis=1)
    places = jnp.clip(layer_of - first_of, 0, teacher_states.shape[0] - 1)
    local = (owner_of == here).astype(jnp.int32)
    rest = jnp.stack([(x + 2) & 3, (x + 1) & 3, (x + 3) & 3, x, zl, valid_counts[0]]).astype(jnp.int32)
    info = jnp.concatenate([places, local, rest])
    near = (owner_of >> 1 == chip).astype(jnp.int32)
    across_near = near[1] == 1

    beyond_slabs = prepare(teacher_states, theirs, info, "beyond")
    y_route = [((i, 0), (i - 1, 0)) for i in range(1, 4)] + [((i, 1), (i + 1, 1)) for i in range(3)]
    y_route = [(a * 2 + b, c * 2 + d) for (a, b), (c, d) in y_route]
    relayed = []
    for chunk in range(2):
        relayed.append(lax.ppermute(beyond_slabs[chunk], ("y", "zh"), y_route))
    across_slabs = prepare(teacher_states, theirs, info, "across")

    def send_across(chunk):
        sent = []
        for k in range(4):
            route = [(h * 4 + z, (1 - h) * 4 + (z + k) % 4) for h in range(2) for z in range(4)]
            slab = jnp.where(across_near, across_slabs[chunk][k], relayed[chunk][k])
            sent.append(lax.ppermute(slab, ("zh", "zl"), route))
        return sent

    def send_own(chunk):
        slabs = here_slabs[4 * chunk : 4 * chunk + 4]
        return [slabs[0]] + [rotate(slabs[k], "zl", k) for k in (1, 2, 3)]

    crossed_first = send_across(0)
    here_slabs = prepare(teacher_states, theirs, info, "here")
    own_first = send_own(0)
    crossed_second = send_across(1)
    own_second = send_own(1)

    rows = jnp.concatenate(students, axis=0)
    w_all = lax.optimization_barrier(jnp.concatenate([w_opp, w_next, w_prev, weights], axis=1))
    projected = lax.optimization_barrier(dot(rows, w_all, 1, 0))
    near = near[2:]
    top, bot = rows[:, :half], rows[:, half:]

    def grad(part, residual):
        return dot(part, residual, 0, 0)

    first_res, squares_first = residual_of(near, projected, own_first, 0, crossed_first)
    opp_res, next_res = first_res[:, :width], first_res[:, width:]
    opp_top = grad(top, opp_res).astype(jnp.bfloat16)
    opp_bot = grad(bot, opp_res).astype(jnp.bfloat16)
    next_bot = grad(bot, next_res).astype(jnp.bfloat16)
    up_top = rotate(opp_top, "x", 1)
    down_bot = rotate(opp_bot, "x", -1)
    second_res, squares_second = residual_of(near, projected, own_second, 1, crossed_second)

    sums = jnp.stack([squares_first[0] + squares_second[0], valid_counts[0].astype(jnp.float32)])
    copies = jnp.broadcast_to(sums, (lax.axis_size(DP), 2))
    sums = jnp.sum(lax.all_to_all(copies, DP, split_axis=0, concat_axis=0, tiled=True), axis=0)
    total = sums[1]
    loss = sums[:1] / (total * (width * lax.axis_size(DP)))
    factor = loss_scale / total

    next_top = (grad(top, next_res) + up_top.astype(jnp.float32)).astype(jnp.bfloat16)
    next_part = lax.optimization_barrier((jnp.concatenate([next_top, next_bot], axis=0), sums))[0]
    from_prev = rotate(next_part, "x", 1)
    prev_res, own_res = second_res[:, :width], second_res[:, width:]
    prev_top = grad(top, prev_res).astype(jnp.bfloat16)
    prev_bot = (grad(bot, prev_res) + down_bot.astype(jnp.float32)).astype(jnp.bfloat16)
    prev_part = lax.optimization_barrier((jnp.concatenate([prev_top, prev_bot], axis=0), sums))[0]
    from_next = rotate(prev_part, "x", -1)

    residual = lax.optimization_barrier(jnp.concatenate([first_res, second_res], axis=1))
    student_part = dot(residual, w_all, 1, 1).astype(jnp.bfloat16)
    student_part = lax.optimization_barrier((student_part, sums))[0]
    returned = []
    for k in (1, 2, 3):
        part = student_part[k * tokens : (k + 1) * tokens]
        returned.append(rotate(part, "zl", -k))
    own_part = lax.optimization_barrier(grad(rows, own_res))

    student_grad = student_part[:tokens].astype(jnp.float32)
    for part in returned:
        student_grad = student_grad + part.astype(jnp.float32)
    student_grad = (student_grad * factor).astype(jnp.bfloat16)
    projector_grad = own_part + from_prev.astype(jnp.float32) + from_next.astype(jnp.float32)
    projector_grad = (projector_grad * factor).astype(jnp.bfloat16)
    return (student_grad[None], projector_grad[None], loss)


def solution(mesh):
    split = Mesh(mesh.devices.reshape(4, 2, 2, 4, 4), SECTION + DP)
    return jax.shard_map(
        compute,
        mesh=split,
        in_specs=(
            P(SECTION, DP, None),
            P(SECTION, DP, None),
            P(SECTION, None, DP),
            P(),
            P(),
            P(DP),
        ),
        out_specs=(P(SECTION, DP, None), P(SECTION, None, DP), P(SECTION)),
        check_vma=False,
    )
```

```python
import functools

import jax
import jax.numpy as jnp
from jax import lax
from jax.experimental import pallas as pl
from jax.experimental.pallas import tpu as pltpu
from jax.sharding import Mesh
from jax.sharding import PartitionSpec as P

loss_scale = 128.0
norm_eps = 1e-06


SECTION = ("y", "zh", "core")
DP = ("x", "zl")
ROWS = 32


def rotate(block, axis, distance):
    n = lax.axis_size(axis)
    return lax.ppermute(block, axis, [(i, (i + distance) % n) for i in range(n)])


def exchange(block, axis, bit):
    n = lax.axis_size(axis)
    return lax.ppermute(block, axis, [(i, i ^ bit) for i in range(n)])


PIECES = ("beyond", "across", "here")
ORDER, ZL, LIMIT = 6, 10, 11


def prepare_body(piece, info, mine, theirs, *refs):
    outs, spread = refs[:-1], refs[-1]
    local = info[3 + piece] == 1
    wide = jnp.where(local, mine[0], theirs[0]).astype(jnp.float32)
    scale = lax.rsqrt(jnp.mean(wide * wide, axis=1, keepdims=True) + norm_eps)
    token = pl.program_id(0) * wide.shape[0] + lax.broadcasted_iota(jnp.int32, scale.shape, 0)
    scale = jnp.where(token < info[LIMIT], scale, 0.0)
    group = wide.shape[1] // 4
    width = group // 4
    for chunk in range(2):
        halves = []
        for half in range(2):
            start = pl.multiple_of(info[ORDER + 2 * chunk + half] * group, group)
            cut = pl.ds(start, group)
            part = jnp.where(local, mine[0, :, cut], theirs[0, :, cut]).astype(jnp.float32)
            halves.append((part * scale).astype(jnp.bfloat16))
        for z in range(4):
            cut = slice(z * width, (z + 1) * width)
            spread[chunk, (z - info[ZL]) & 3] = jnp.concatenate([h[:, cut] for h in halves], axis=1)
    for index, out in enumerate(outs):
        out[...] = spread[index // 4, index % 4] if PIECES[piece] == "here" else spread[index]


def prepare(mine, theirs, info, name):
    _, tokens, features = mine.shape
    piece = PIECES.index(name)
    rows = min(ROWS, tokens)
    wide = features // 8
    lead = [()] * 8 if name == "here" else [(4,)] * 2

    def taken(kept):
        def index(i, info):
            on = info[3 + piece] if kept else 1 - info[3 + piece]
            return (info[piece] * on, i * on, 0)

        return pl.BlockSpec((1, rows, features), index)

    def written(dims):
        return pl.BlockSpec((*dims, rows, wide), lambda i, info: (0,) * len(dims) + (i, 0))

    return pl.pallas_call(
        functools.partial(prepare_body, piece),
        out_shape=[jax.ShapeDtypeStruct((*dims, tokens, wide), jnp.bfloat16) for dims in lead],
        grid_spec=pltpu.PrefetchScalarGridSpec(
            num_scalar_prefetch=1,
            grid=(tokens // rows,),
            in_specs=[taken(True), taken(False)],
            out_specs=[written(dims) for dims in lead],
            scratch_shapes=[pltpu.VMEM((2, 4, rows, wide), jnp.bfloat16)],
        ),
        compiler_params=pltpu.CompilerParams(dimension_semantics=("arbitrary",), vmem_limit_bytes=58 << 20),
    )(info, mine, theirs)


def residual_body(near, projected, *refs):
    own, cross, (out, squares) = refs[:4], refs[4:8], refs[8:]
    rows = cross[0].shape[0]
    total = jnp.zeros((), jnp.float32)
    for k in range(4):
        cut = slice(k * rows, (k + 1) * rows)
        target = jnp.where(near[0] == 1, own[k][...].astype(jnp.float32), cross[k][...].astype(jnp.float32))
        residual = projected[cut] - target
        out[cut] = residual.astype(jnp.bfloat16)
        total = total + jnp.sum(residual * residual)
    squares[0] = total


def residual_of(near, projected, own, chunk, cross):
    tokens = projected.shape[0]
    rows, wide = cross[0].shape

    def whole(shape):
        return pl.BlockSpec(shape, lambda i: (0, 0))

    smem = pl.BlockSpec(memory_space=pltpu.SMEM)
    return pl.pallas_call(
        residual_body,
        out_shape=(
            jax.ShapeDtypeStruct((tokens, wide), jnp.bfloat16),
            jax.ShapeDtypeStruct((1,), jnp.float32),
        ),
        grid=(1,),
        in_specs=[smem, pl.BlockSpec((tokens, wide), lambda i: (0, chunk))]
        + [whole((rows, wide))] * 8,
        out_specs=(whole((tokens, wide)), smem),
        compiler_params=pltpu.CompilerParams(vmem_limit_bytes=16 << 20),
    )(near, projected, *own, *cross)


def dot(a, b, ca, cb):
    return lax.dot_general(a, b, (((ca,), (cb,)), ((), ())), preferred_element_type=jnp.float32)


def compute(student_states, teacher_states, projector, layer_map, boundaries, valid_counts):
    y, zh, core = (lax.axis_index(a) for a in SECTION)
    x, zl = (lax.axis_index(a) for a in DP)
    sections = lax.axis_size(SECTION)
    chip = 2 * y + zh
    here = 2 * chip + core
    weights = projector[0]
    tokens = student_states.shape[1]
    width = weights.shape[1]

    theirs = exchange(teacher_states, "core", 1)

    valid = lax.broadcasted_iota(jnp.int32, (tokens, 1), 0) < valid_counts[0]
    student = jnp.where(valid, student_states[0], 0)
    students = [student]
    for k in (1, 2, 3):
        students.append(rotate(student, "zl", k))
    w_prev = rotate(weights, "x", 1)
    w_next = rotate(weights, "x", -1)
    w_opp = rotate(weights, "x", 2)

    owners = jnp.sum((boundaries[None, 1:sections] <= layer_map[:, None]).astype(jnp.int32), axis=1)
    layers = jnp.arange(sections, dtype=jnp.int32)
    across = 2 * (2 * y + 1 - zh) + core
    beyond = jnp.where(zh == 0, 2 * (chip - 1), 2 * (chip + 1)) + core
    wanted = jnp.stack([beyond, across, here])
    hit = layers[None, :] == wanted[:, None]
    owner_of = jnp.sum(jnp.where(hit, owners[None, :], 0), axis=1)
    layer_of = jnp.sum(jnp.where(hit, layer_map[None, :], 0), axis=1)
    first_of = jnp.sum(jnp.where(layers[None, :] == owner_of[:, None], boundaries[None, :sections], 0), axis=1)
    places = jnp.clip(layer_of - first_of, 0, teacher_states.shape[0] - 1)
    local = (owner_of == here).astype(jnp.int32)
    rest = jnp.stack([(x + 2) & 3, (x + 1) & 3, (x + 3) & 3, x, zl, valid_counts[0]]).astype(jnp.int32)
    info = jnp.concatenate([places, local, rest])
    near = (owner_of >> 1 == chip).astype(jnp.int32)
    across_near = near[1] == 1

    beyond_slabs = prepare(teacher_states, theirs, info, "beyond")
    y_route = [((i, 0), (i - 1, 0)) for i in range(1, 4)] + [((i, 1), (i + 1, 1)) for i in range(3)]
    y_route = [(a * 2 + b, c * 2 + d) for (a, b), (c, d) in y_route]
    relayed = []
    for chunk in range(2):
        relayed.append(lax.ppermute(beyond_slabs[chunk], ("y", "zh"), y_route))
    across_slabs = prepare(teacher_states, theirs, info, "across")

    def send_across(chunk):
        sent = []
        for k in range(4):
            route = [(h * 4 + z, (1 - h) * 4 + (z + k) % 4) for h in range(2) for z in range(4)]
            slab = jnp.where(across_near, across_slabs[chunk][k], relayed[chunk][k])
            sent.append(lax.ppermute(slab, ("zh", "zl"), route))
        return sent

    def send_own(chunk):
        slabs = here_slabs[4 * chunk : 4 * chunk + 4]
        return [slabs[0]] + [rotate(slabs[k], "zl", k) for k in (1, 2, 3)]

    crossed_first = send_across(0)
    here_slabs = prepare(teacher_states, theirs, info, "here")
    own_first = send_own(0)
    crossed_second = send_across(1)
    own_second = send_own(1)

    rows = lax.optimization_barrier(jnp.concatenate(students, axis=0))
    w_all = lax.optimization_barrier(jnp.concatenate([w_opp, w_next, w_prev, weights], axis=1))
    projected = lax.optimization_barrier(dot(rows, w_all, 1, 0))
    near = near[2:]

    def grad(residual):
        return dot(rows, residual, 0, 0)

    first_res, squares_first = residual_of(near, projected, own_first, 0, crossed_first)
    opp_part = grad(first_res[:, :width])
    from_opp = rotate(opp_part.astype(jnp.bfloat16), "x", 2)
    next_part = lax.optimization_barrier(grad(first_res[:, width:]).astype(jnp.bfloat16))
    part_first = lax.optimization_barrier(dot(first_res, w_all[:, : 2 * width], 1, 1))
    second_res, squares_second = residual_of(near, projected, own_second, 1, crossed_second)
    student_part = (part_first + dot(second_res, w_all[:, 2 * width :], 1, 1)).astype(jnp.bfloat16)
    parts = [student_part[k * tokens : (k + 1) * tokens] for k in range(4)]
    prev_part = grad(second_res[:, :width]).astype(jnp.bfloat16)

    sums = jnp.stack([squares_first[0] + squares_second[0], valid_counts[0].astype(jnp.float32)])
    sums, parts, prev_part = lax.optimization_barrier((sums, parts, prev_part))
    copies = jnp.broadcast_to(sums, (lax.axis_size(DP), 2))
    sums = jnp.sum(lax.all_to_all(copies, DP, split_axis=0, concat_axis=0, tiled=True), axis=0)
    sums, parts, prev_part, next_part = lax.optimization_barrier((sums, parts, prev_part, next_part))
    total = sums[1]
    loss = sums[:1] / (total * (width * lax.axis_size(DP)))
    factor = loss_scale / total

    returned = []
    for k in (1, 2, 3):
        returned.append(rotate(parts[k], "zl", -k))
    from_next = rotate(prev_part, "x", -1)
    from_prev = rotate(next_part, "x", 1)
    own_part = lax.optimization_barrier(grad(second_res[:, width:]))

    student_grad = parts[0].astype(jnp.float32)
    for part in returned:
        student_grad = student_grad + part.astype(jnp.float32)
    student_grad = (student_grad * factor).astype(jnp.bfloat16)
    projector_grad = own_part
    for part in (from_prev, from_next, from_opp):
        projector_grad = projector_grad + part.astype(jnp.float32)
    projector_grad = (projector_grad * factor).astype(jnp.bfloat16)
    return (student_grad[None], projector_grad[None], loss)


def solution(mesh):
    split = Mesh(mesh.devices.reshape(4, 2, 2, 4, 4), SECTION + DP)
    return jax.shard_map(
        compute,
        mesh=split,
        in_specs=(
            P(SECTION, DP, None),
            P(SECTION, DP, None),
            P(SECTION, None, DP),
            P(),
            P(),
            P(DP),
        ),
        out_specs=(P(SECTION, DP, None), P(SECTION, None, DP), P(SECTION)),
        check_vma=False,
    )
```

```python
import functools

import jax
import jax.numpy as jnp
from jax import lax
from jax.experimental import pallas as pl
from jax.experimental.pallas import tpu as pltpu
from jax.sharding import Mesh
from jax.sharding import PartitionSpec as P

loss_scale = 128.0
norm_eps = 1e-06


SECTION = ("y", "zh", "core")
DP = ("x", "zl")
ROWS = 32


def rotate(block, axis, distance):
    n = lax.axis_size(axis)
    return lax.ppermute(block, axis, [(i, (i + distance) % n) for i in range(n)])


def exchange(block, axis, bit):
    n = lax.axis_size(axis)
    return lax.ppermute(block, axis, [(i, i ^ bit) for i in range(n)])


PIECES = ("beyond", "across", "here")
ORDER, ZL, LIMIT = 6, 10, 11


def prepare_body(piece, info, mine, theirs, *refs):
    outs, spread = refs[:-1], refs[-1]
    local = info[3 + piece] == 1
    wide = jnp.where(local, mine[0], theirs[0]).astype(jnp.float32)
    scale = lax.rsqrt(jnp.mean(wide * wide, axis=1, keepdims=True) + norm_eps)
    token = pl.program_id(0) * wide.shape[0] + lax.broadcasted_iota(jnp.int32, scale.shape, 0)
    scale = jnp.where(token < info[LIMIT], scale, 0.0)
    group = wide.shape[1] // 4
    width = group // 4
    for chunk in range(2):
        halves = []
        for half in range(2):
            start = pl.multiple_of(info[ORDER + 2 * chunk + half] * group, group)
            cut = pl.ds(start, group)
            part = jnp.where(local, mine[0, :, cut], theirs[0, :, cut]).astype(jnp.float32)
            halves.append((part * scale).astype(jnp.bfloat16))
        for z in range(4):
            cut = slice(z * width, (z + 1) * width)
            spread[chunk, (z - info[ZL]) & 3] = jnp.concatenate([h[:, cut] for h in halves], axis=1)
    for index, out in enumerate(outs):
        out[...] = spread[index // 4, index % 4] if PIECES[piece] == "here" else spread[index]


def prepare(mine, theirs, info, name):
    _, tokens, features = mine.shape
    piece = PIECES.index(name)
    rows = min(ROWS, tokens)
    wide = features // 8
    lead = [()] * 8 if name == "here" else [(4,)] * 2

    def taken(kept):
        def index(i, info):
            on = info[3 + piece] if kept else 1 - info[3 + piece]
            return (info[piece] * on, i * on, 0)

        return pl.BlockSpec((1, rows, features), index)

    def written(dims):
        return pl.BlockSpec((*dims, rows, wide), lambda i, info: (0,) * len(dims) + (i, 0))

    return pl.pallas_call(
        functools.partial(prepare_body, piece),
        out_shape=[jax.ShapeDtypeStruct((*dims, tokens, wide), jnp.bfloat16) for dims in lead],
        grid_spec=pltpu.PrefetchScalarGridSpec(
            num_scalar_prefetch=1,
            grid=(tokens // rows,),
            in_specs=[taken(True), taken(False)],
            out_specs=[written(dims) for dims in lead],
            scratch_shapes=[pltpu.VMEM((2, 4, rows, wide), jnp.bfloat16)],
        ),
        compiler_params=pltpu.CompilerParams(dimension_semantics=("arbitrary",), vmem_limit_bytes=58 << 20),
    )(info, mine, theirs)


def residual_body(chunk, near, projected, *refs):
    own, cross, earlier, (out, squares) = refs[:4], refs[4:8], refs[8:-2], refs[-2:]
    rows, wide = cross[0].shape
    left = chunk * wide
    for ref in earlier:
        out[:, :left] = ref[...]
    total = jnp.zeros((), jnp.float32)
    for k in range(4):
        cut = slice(k * rows, (k + 1) * rows)
        target = jnp.where(near[0] == 1, own[k][...].astype(jnp.float32), cross[k][...].astype(jnp.float32))
        residual = projected[cut] - target
        out[cut, left:] = residual.astype(jnp.bfloat16)
        total = total + jnp.sum(residual * residual)
    squares[0] = total


def residual_of(near, projected, own, chunk, cross, *earlier):
    tokens = projected.shape[0]
    rows, wide = cross[0].shape

    def whole(shape):
        return pl.BlockSpec(shape, lambda i: (0, 0))

    smem = pl.BlockSpec(memory_space=pltpu.SMEM)
    return pl.pallas_call(
        functools.partial(residual_body, chunk),
        out_shape=(
            jax.ShapeDtypeStruct((tokens, (chunk + 1) * wide), jnp.bfloat16),
            jax.ShapeDtypeStruct((1,), jnp.float32),
        ),
        grid=(1,),
        in_specs=[smem, pl.BlockSpec((tokens, wide), lambda i: (0, chunk))]
        + [whole((rows, wide))] * 8
        + [whole((tokens, wide))] * chunk,
        out_specs=(whole((tokens, (chunk + 1) * wide)), smem),
        compiler_params=pltpu.CompilerParams(vmem_limit_bytes=16 << 20),
    )(near, projected, *own, *cross, *earlier)


def dot(a, b, ca, cb):
    return lax.dot_general(a, b, (((ca,), (cb,)), ((), ())), preferred_element_type=jnp.float32)


def compute(student_states, teacher_states, projector, layer_map, boundaries, valid_counts):
    y, zh, core = (lax.axis_index(a) for a in SECTION)
    x, zl = (lax.axis_index(a) for a in DP)
    sections = lax.axis_size(SECTION)
    chip = 2 * y + zh
    here = 2 * chip + core
    weights = projector[0]
    tokens = student_states.shape[1]
    half = weights.shape[0] // 2
    width = weights.shape[1]

    theirs = exchange(teacher_states, "core", 1)

    valid = lax.broadcasted_iota(jnp.int32, (tokens, 1), 0) < valid_counts[0]
    student = jnp.where(valid, student_states[0], 0)
    students = [student]
    for k in (1, 2, 3):
        students.append(rotate(student, "zl", k))
    w_prev = rotate(weights, "x", 1)
    w_next = rotate(weights, "x", -1)
    w_opp = rotate(weights, "x", 2)

    owners = jnp.sum((boundaries[None, 1:sections] <= layer_map[:, None]).astype(jnp.int32), axis=1)
    layers = jnp.arange(sections, dtype=jnp.int32)
    across = 2 * (2 * y + 1 - zh) + core
    beyond = jnp.where(zh == 0, 2 * (chip - 1), 2 * (chip + 1)) + core
    wanted = jnp.stack([beyond, across, here])
    hit = layers[None, :] == wanted[:, None]
    owner_of = jnp.sum(jnp.where(hit, owners[None, :], 0), axis=1)
    layer_of = jnp.sum(jnp.where(hit, layer_map[None, :], 0), axis=1)
    first_of = jnp.sum(jnp.where(layers[None, :] == owner_of[:, None], boundaries[None, :sections], 0), axis=1)
    places = jnp.clip(layer_of - first_of, 0, teacher_states.shape[0] - 1)
    local = (owner_of == here).astype(jnp.int32)
    rest = jnp.stack([(x + 2) & 3, (x + 1) & 3, (x + 3) & 3, x, zl, valid_counts[0]]).astype(jnp.int32)
    info = jnp.concatenate([places, local, rest])
    near = (owner_of >> 1 == chip).astype(jnp.int32)
    across_near = near[1] == 1

    beyond_slabs = prepare(teacher_states, theirs, info, "beyond")
    y_route = [((i, 0), (i - 1, 0)) for i in range(1, 4)] + [((i, 1), (i + 1, 1)) for i in range(3)]
    y_route = [(a * 2 + b, c * 2 + d) for (a, b), (c, d) in y_route]
    relayed = []
    for chunk in range(2):
        relayed.append(lax.ppermute(beyond_slabs[chunk], ("y", "zh"), y_route))
    across_slabs = prepare(teacher_states, theirs, info, "across")

    def send_across(chunk):
        sent = []
        for k in range(4):
            route = [(h * 4 + z, (1 - h) * 4 + (z + k) % 4) for h in range(2) for z in range(4)]
            slab = jnp.where(across_near, across_slabs[chunk][k], relayed[chunk][k])
            sent.append(lax.ppermute(slab, ("zh", "zl"), route))
        return sent

    def send_own(chunk):
        slabs = here_slabs[4 * chunk : 4 * chunk + 4]
        return [slabs[0]] + [rotate(slabs[k], "zl", k) for k in (1, 2, 3)]

    crossed_first = send_across(0)
    here_slabs = prepare(teacher_states, theirs, info, "here")
    own_first = send_own(0)
    crossed_second = send_across(1)
    own_second = send_own(1)

    rows = lax.optimization_barrier(jnp.concatenate(students, axis=0))
    w_all = lax.optimization_barrier(jnp.concatenate([w_opp, w_next, w_prev, weights], axis=1))
    projected = lax.optimization_barrier(dot(rows, w_all, 1, 0))
    near = near[2:]

    def grad(residual):
        return dot(rows, residual, 0, 0)

    first_res, squares_first = residual_of(near, projected, own_first, 0, crossed_first)
    opp_part = grad(first_res[:, :width]).astype(jnp.bfloat16)
    up_top = rotate(opp_part[:half], "x", 1)
    down_bot = rotate(opp_part[half:], "x", -1)
    next_part = lax.optimization_barrier(grad(first_res[:, width:]).astype(jnp.bfloat16))
    residual, squares_second = residual_of(near, projected, own_second, 1, crossed_second, first_res)
    student_part = dot(residual, w_all, 1, 1).astype(jnp.bfloat16)
    parts = [student_part[k * tokens : (k + 1) * tokens] for k in range(4)]
    prev_part = grad(residual[:, 2 * width : 3 * width])

    def plus(part, arrived, low, high):
        padded = jnp.pad(arrived.astype(jnp.float32), ((low, high), (0, 0)))
        return (part.astype(jnp.float32) + padded).astype(jnp.bfloat16)

    next_part = plus(next_part, up_top, 0, half)
    prev_part = plus(prev_part, down_bot, half, 0)

    sums = jnp.stack([squares_first[0] + squares_second[0], valid_counts[0].astype(jnp.float32)])
    for axis in ("zl", "x"):
        sums = sums + exchange(sums, axis, 1)
        sums = sums + exchange(sums, axis, 2)
    total = sums[1]
    loss = sums[:1] / (total * (width * lax.axis_size(DP)))
    factor = loss_scale / total

    returned = []
    for k in (1, 2, 3):
        returned.append(rotate(parts[k], "zl", -k))
    from_next = rotate(prev_part, "x", -1)
    from_prev = rotate(next_part, "x", 1)
    own_part = lax.optimization_barrier(grad(residual[:, 3 * width :]))

    student_grad = parts[0].astype(jnp.float32)
    for part in returned:
        student_grad = student_grad + part.astype(jnp.float32)
    student_grad = (student_grad * factor).astype(jnp.bfloat16)
    projector_grad = own_part
    for part in (from_prev, from_next):
        projector_grad = projector_grad + part.astype(jnp.float32)
    projector_grad = (projector_grad * factor).astype(jnp.bfloat16)[None]
    return (student_grad[None], projector_grad, loss)


def solution(mesh):
    split = Mesh(mesh.devices.reshape(4, 2, 2, 4, 4), SECTION + DP)
    return jax.shard_map(
        compute,
        mesh=split,
        in_specs=(
            P(SECTION, DP, None),
            P(SECTION, DP, None),
            P(SECTION, None, DP),
            P(),
            P(),
            P(DP),
        ),
        out_specs=(P(SECTION, DP, None), P(SECTION, None, DP), P(SECTION)),
        check_vma=False,
    )
```
